32 devices in a mesh: tile: 8 (over y, x, core), bulk: 4 (over z).
Axes of the slice: x: 2, y: 2, z: 4, core: 2. Of those that a mesh axis runs over, the one named last changes fastest.
Arguments:
- integrals: bfloat16 [96, 256, 768], P(('tile', 'bulk')), may hold values from -0.21875 to 0.21875
- amplitudes: bfloat16 [4, 768, 1024], P(None, 'bulk', 'tile'), may hold values from -6 to 6
- residual_in: bfloat16 [96, 256, 1024], P(('tile', 'bulk')), may hold values from -6 to 6
- tile_irrep: int32 [96], replicated, may hold values from 0 to 3, as said below
Outputs:
- residual: bfloat16 [96, 256, 1024], P(('tile', 'bulk'))
The draws below stay inside these ranges and needn't reach their ends.
Inputs may be any that keep to these rules, and one draw needn't show every extreme that they name: tile_irrep never falls along the tiles, and every irrep labels at least 12 tiles.
All inputs are finite; a program needn't handle non-finite values.
Results may differ from the reference program's by a relative error of at most 0.001.
Values may be sent and summed in bfloat16 or wider, within the bound.
A program may use at most 64 MiB of HBM per device.

```python
import jax
import jax.numpy as jnp
from jax import lax

V = 768
PP = 1024
IRREPS = 4
TILE = 256
ROW_TILES = 12
NT = 96


def draw_tile_irrep(key, part):
    spare_tiles = NT - 4 * ROW_TILES
    cut_points = jnp.sort(jax.random.randint(key, (3,), 0, spare_tiles + 1))
    bounds = cut_points.astype(jnp.int32) + ROW_TILES * jnp.arange(1, 4, dtype=jnp.int32)
    positions = jnp.arange(NT, dtype=jnp.int32)
    return jnp.sum((positions[:, None] >= bounds[None, :]).astype(jnp.int32), axis=1).astype(jnp.int32)


def block_levels(key, dims, shards, smallest, largest):
    factor_of = 1.0
    for position, blocks in shards:
        steps = jax.random.uniform(jax.random.fold_in(jax.random.fold_in(key, 6), position), (blocks,), jnp.float32, smallest / len(shards), largest / len(shards))
        factor_of = factor_of * jnp.repeat(jnp.exp(steps), dims[position] // blocks).reshape((-1,) + (1,) * (len(dims) - 1 - position))
    return factor_of


def normal_values(rng, extent, scale, limit, cuts=(), held_as=jnp.bfloat16):
    array = scale * jax.random.normal(rng, extent, jnp.float32)
    if cuts:
        array = array * block_levels(rng, extent, cuts, -0.22, 0.18)
    return jnp.clip(array, -limit, limit).astype(held_as)


def setup_inputs(seed: int = 0) -> dict:
    arg_keys = jax.random.split(jax.random.key(seed), 5)
    return {
        "integrals": normal_values(arg_keys[0], (NT, TILE, V), V ** -0.5, 0.21875, ((0, 32),)),
        "amplitudes": normal_values(arg_keys[1], (IRREPS, V, PP), 1.0, 6.0, ((1, 4), (2, 8))),
        "residual_in": normal_values(arg_keys[2], (NT, TILE, PP), 1.0, 6.0, ((0, 32),)),
        "tile_irrep": draw_tile_irrep(jax.random.fold_in(arg_keys[4], 71), 0),
    }


def reference(integrals, amplitudes, residual_in, tile_irrep):
    def one_tile(operands):
        block, previous, irrep = operands
        chosen = lax.dynamic_index_in_dim(amplitudes, irrep, 0, keepdims=False)
        ladder = jnp.dot(block, chosen, preferred_element_type=jnp.float32)
        return (previous.astype(jnp.float32) + ladder).astype(jnp.bfloat16)

    return lax.map(one_tile, (integrals, residual_in, tile_irrep))
```

```python
import functools

import jax
import jax.numpy as jnp
from jax import lax
from jax.experimental import pallas as pl
from jax.experimental.pallas import tpu as pltpu
from jax.sharding import PartitionSpec as P

MESH = pl.DeviceIdType.MESH
PARTS = 2
VMEM_LIMIT = 32 << 20


def gathered_plan(integrals, amplitudes, residual_in, tile_irrep):
    tile_dev = integrals.shape[0]
    first_tile = (lax.axis_index("tile") * lax.axis_size("bulk") + lax.axis_index("bulk")) * tile_dev
    local_irrep = lax.dynamic_slice_in_dim(tile_irrep, first_tile, tile_dev, 0)
    whole_cd = lax.all_gather(amplitudes, "bulk", axis=1, tiled=True)
    picked = jnp.take(lax.all_gather(whole_cd, "tile", axis=2, tiled=True), local_irrep, axis=0)
    product = jnp.einsum("trc,tcp->trp", integrals, picked, preferred_element_type=jnp.float32)
    return (residual_in.astype(jnp.float32) + product).astype(jnp.bfloat16)


def kernel(rows, bulk, slots, parts, irrep_hbm, amp_hbm, int_hbm, res_hbm, out_ref, flag_ref, *scratch):
    cols = rows // 2
    offsets = [0] + [s * d for d in range(1, bulk) for s in (-1, 1)]
    chunks = len(offsets)
    (irrep_ref, amp, ints, res, lhs, total), scratch = scratch[:6], scratch[6:]
    gathered, scratch = [scratch[:chunks], scratch[chunks:2 * chunks]], scratch[2 * chunks:]
    held = [[None] * parts] + [list(scratch[i * parts:(i + 1) * parts]) for i in range(chunks - 1)]
    scratch = scratch[(chunks - 1) * parts:]
    picked = [list(scratch[i * parts:(i + 1) * parts]) for i in range(chunks)]
    (z_send, z_recv, c_send, c_recv, p_send, p_recv, local_sem) = scratch[chunks * parts:]
    tiles = ints.shape[0]
    irreps, depth, width = amp.shape
    piece = depth // parts
    me, at = lax.axis_index("tile"), lax.axis_index("bulk")
    col, core = me // 2, me % 2
    partner = col * 2 + (1 - core)

    irrep_copy = pltpu.make_async_copy(irrep_hbm, irrep_ref, local_sem.at[3])
    amp_copy = pltpu.make_async_copy(amp_hbm, amp, local_sem.at[0])
    int_copy = pltpu.make_async_copy(int_hbm, ints, local_sem.at[1])
    res_copy = pltpu.make_async_copy(res_hbm, res, local_sem.at[2])
    amp_copy.start()
    irrep_copy.start()

    barrier = pltpu.get_barrier_semaphore()
    pl.semaphore_signal(barrier, inc=1, device_id=(partner, at), device_id_type=MESH)
    for j in range(1, cols):
        pl.semaphore_signal(barrier, inc=1, device_id=(lax.rem(col + j, cols) * 2 + core, at), device_id_type=MESH)

    @pl.when(at > 0)
    def _():
        pl.semaphore_signal(barrier, inc=1, device_id=(me, at - 1), device_id_type=MESH)

    @pl.when(at < bulk - 1)
    def _():
        pl.semaphore_signal(barrier, inc=1, device_id=(me, at + 1), device_id_type=MESH)

    int_copy.start()
    res_copy.start()
    pl.semaphore_wait(barrier, cols + (at > 0).astype(jnp.int32) + (at < bulk - 1).astype(jnp.int32))

    amp_copy.wait()

    def block(c, p):
        if c == 0:
            return amp.at[:, pl.ds(p * piece, piece), :]
        return held[c][p]

    def line(c, p, step):
        there = offsets.index(offsets[c] - step)
        way = 0 if step > 0 else 1
        return pltpu.make_async_remote_copy(
            src_ref=block(c, p), dst_ref=held[there][p], send_sem=z_send.at[way, c, p],
            recv_sem=z_recv.at[there, p], device_id=(me, at + step), device_id_type=MESH)

    def line_in(c, p):
        return pltpu.make_async_remote_copy(
            src_ref=held[c][p], dst_ref=held[c][p], send_sem=z_send.at[0, c, p],
            recv_sem=z_recv.at[c, p], device_id=(partner, at), device_id_type=MESH)

    def slab(side, c, p, column):
        return gathered[side][c].at[:, pl.ds(p * piece, piece), pl.ds(pl.multiple_of(column * width, 128), width)]

    def across(c, p, j):
        return pltpu.make_async_remote_copy(
            src_ref=picked[c][p].at[j - 1], dst_ref=slab(0, c, p, col), send_sem=c_send.at[c, p, j],
            recv_sem=c_recv.at[c, p, j], device_id=(lax.rem(col + j, cols) * 2 + core, at), device_id_type=MESH)

    def over(c, p, j):
        column = lax.rem(col - j + cols, cols)
        return pltpu.make_async_remote_copy(
            src_ref=slab(0, c, p, column), dst_ref=slab(1, c, p, column), send_sem=p_send.at[c, p, j],
            recv_sem=p_recv.at[c, p, j], device_id=(partner, at), device_id_type=MESH)

    def wanted(column):
        low = (2 * column * bulk + at) * tiles
        high = ((2 * column + 1) * bulk + at) * tiles + tiles - 1
        spots = [low, high] if slots == 2 else [low, low + tiles - 1, high]
        return [irrep_ref[s] for s in spots]

    def present(c):
        src = at + offsets[c]
        return jnp.logical_and(src >= 0, src < bulk)

    def relay(c, p):
        if offsets[c] <= 0:
            @pl.when(at < bulk - 1)
            def _():
                line(c, p, 1).start()
        if offsets[c] >= 0:
            @pl.when(at > 0)
            def _():
                line(c, p, -1).start()

    def relay_done(c, p):
        if offsets[c] <= 0 and offsets[c] - 1 > -bulk:
            @pl.when(at < bulk - 1)
            def _():
                line(c, p, 1).wait_send()
        if offsets[c] >= 0 and offsets[c] + 1 < bulk:
            @pl.when(at > 0)
            def _():
                line(c, p, -1).wait_send()

    def spread(c, p):
        src = amp if c == 0 else held[c][p]
        lanes = pl.ds(p * piece, piece) if c == 0 else slice(None)
        for j in range(1, cols):
            for s, g in enumerate(wanted(lax.rem(col + j, cols))):
                picked[c][p][j - 1, s] = src[g, lanes, :]
            across(c, p, j).start()
        for s, g in enumerate(wanted(col)):
            gathered[0][c][s, pl.ds(p * piece, piece), pl.ds(pl.multiple_of(col * width, 128), width)] = src[g, lanes, :]
        over(c, p, 0).start()

    def forward(c, p):
        for j in range(1, cols):
            landed = slab(0, c, p, lax.rem(col - j + cols, cols))
            pltpu.make_async_remote_copy(
                src_ref=landed, dst_ref=landed, send_sem=c_send.at[c, p, j], recv_sem=c_recv.at[c, p, j],
                device_id=(partner, at), device_id_type=MESH).wait_recv()
            over(c, p, j).start()

    first_tile = (me * bulk + at) * tiles
    half = cols * width
    last = jnp.where(2 * at < bulk, bulk - 1, 0)

    def arrived(c):
        for p in range(parts):
            for j in range(cols):
                over(c, p, j).wait_recv()

    def product(c, side, begin, end):
        def one(t):
            irrep = irrep_ref[first_tile + t]
            slot = (irrep > mine[0]).astype(jnp.int32)
            for s in mine[1:-1]:
                slot = slot + (irrep > s).astype(jnp.int32)
            part = jnp.dot(lhs[at + offsets[c], t], gathered[side][c][slot], preferred_element_type=jnp.float32)
            if not begin:
                part = part + total[side, t]
            if not begin and not end:
                total[side, t] = part
                return
            for n in range(cols):
                there = pl.ds(pl.multiple_of((n * 2 + (core if side == 0 else 1 - core)) * width, width), width)
                here = part[:, n * width:(n + 1) * width]
                if end:
                    out_ref[t, :, there] = here.astype(jnp.bfloat16)
                else:
                    total[side, t, :, n * width:(n + 1) * width] = here + res[t, :, there].astype(jnp.float32)

        for t in range(tiles):
            one(t)

    groups = [[0]] + [[2 * d - 1, 2 * d] for d in range(1, bulk)]

    def add(d):
        for c in groups[d]:
            src = at + offsets[c]

            @pl.when(jnp.logical_and(present(c), src != last))
            def _():
                arrived(c)
                for side in range(2):
                    product(c, side, d == 0, False)

    def gather(d):
        for p in range(parts):
            for c in groups[d]:
                @pl.when(present(c))
                def _():
                    forward(c, p)

    for p in range(parts):
        relay(0, p)
    irrep_copy.wait()
    mine = wanted(col)
    for p in range(parts):
        spread(0, p)
    third = jnp.int32(0)
    for column in range(cols):
        for plane in range(bulk):
            low = irrep_ref[(2 * column * bulk + plane) * tiles]
            high = irrep_ref[((2 * column + 1) * bulk + plane) * tiles + tiles - 1]
            third = third + (high > low + 1).astype(jnp.int32)
    flag_ref[0] = third
    int_copy.wait()
    for k in range(bulk):
        for t in range(tiles):
            lhs[k, t] = ints[t, :, k * depth:(k + 1) * depth]
    res_copy.wait()
    for d in range(1, bulk):
        for p in range(parts):
            for c in groups[d]:
                @pl.when(present(c))
                def _():
                    line_in(c, p).wait_recv()
                    if d < bulk - 1:
                        relay(c, p)
                    spread(c, p)
        if d >= 2:
            add(d - 2)
        gather(d - 1)
    add(bulk - 2)
    gather(bulk - 1)
    for c in range(1, chunks):
        if 2 * abs(offsets[c]) >= bulk:
            @pl.when(at + offsets[c] == last)
            def _():
                product(c, 0, False, True)
                arrived(c)
                product(c, 1, False, True)

    for group in groups:
        for c in group:
            @pl.when(present(c))
            def _():
                for p in range(parts):
                    for j in range(cols):
                        over(c, p, j).wait_send()
                    for j in range(1, cols):
                        across(c, p, j).wait_send()
                    relay_done(c, p)


def call(rows, bulk, slots, integrals, amplitudes, residual_in, tile_irrep):
    irreps, depth, width = amplitudes.shape
    parts = PARTS if depth % (16 * PARTS) == 0 else 1
    chunks = 2 * bulk - 1
    cols = rows // 2
    any_space = pl.BlockSpec(memory_space=pltpu.HBM)
    return pl.pallas_call(
        functools.partial(kernel, rows, bulk, slots, parts),
        out_shape=(
            jax.ShapeDtypeStruct(residual_in.shape, residual_in.dtype),
            jax.ShapeDtypeStruct((1,), jnp.int32),
        ),
        in_specs=[any_space] * 4,
        out_specs=(pl.BlockSpec(memory_space=pltpu.VMEM), pl.BlockSpec(memory_space=pltpu.SMEM)),
        scratch_shapes=[
            pltpu.SMEM(tile_irrep.shape, tile_irrep.dtype),
            pltpu.VMEM(amplitudes.shape, amplitudes.dtype),
            pltpu.VMEM(integrals.shape, integrals.dtype),
            pltpu.VMEM(residual_in.shape, residual_in.dtype),
            pltpu.VMEM((bulk, *integrals.shape[:2], depth), integrals.dtype),
            pltpu.VMEM((2, *residual_in.shape[:2], cols * width), jnp.float32),
            *[pltpu.VMEM((slots, depth, cols * width), amplitudes.dtype)] * (2 * chunks),
            *[pltpu.VMEM((irreps, depth // parts, width), amplitudes.dtype)] * ((chunks - 1) * parts),
            *[pltpu.VMEM((cols - 1, slots, depth // parts, width), amplitudes.dtype)] * (chunks * parts),
            pltpu.SemaphoreType.DMA((2, chunks, parts)),
            pltpu.SemaphoreType.DMA((chunks, parts)),
            pltpu.SemaphoreType.DMA((chunks, parts, cols)),
            pltpu.SemaphoreType.DMA((chunks, parts, cols)),
            pltpu.SemaphoreType.DMA((chunks, parts, cols)),
            pltpu.SemaphoreType.DMA((chunks, parts, cols)),
            pltpu.SemaphoreType.DMA((4,)),
        ],
        compiler_params=pltpu.CompilerParams(collective_id=slots, has_side_effects=True, vmem_limit_bytes=VMEM_LIMIT),
    )(tile_irrep, amplitudes, integrals, residual_in)


def local(rows, bulk, integrals, amplitudes, residual_in, tile_irrep):
    depth, width = amplitudes.shape[1:]
    if rows % 2 or rows < 4 or bulk < 2 or depth % 16 or width % 128:
        return gathered_plan(integrals, amplitudes, residual_in, tile_irrep)
    out, third = call(rows, bulk, 2, integrals, amplitudes, residual_in, tile_irrep)
    return lax.cond(
        third[0] > 0,
        lambda out, *args: call(rows, bulk, 3, *args)[0],
        lambda out, *args: out,
        out, integrals, amplitudes, residual_in, tile_irrep)


def solution(mesh):
    return jax.shard_map(
        functools.partial(local, mesh.shape["tile"], mesh.shape["bulk"]),
        mesh=mesh,
        in_specs=(
            P(("tile", "bulk"), None, None),
            P(None, "bulk", "tile"),
            P(("tile", "bulk"), None, None),
            P(),
        ),
        out_specs=P(("tile", "bulk"), None, None),
        check_vma=False,
    )
```

```python
import functools

import jax
import jax.numpy as jnp
from jax import lax
from jax.experimental import pallas as pl
from jax.experimental.pallas import tpu as pltpu
from jax.sharding import PartitionSpec as P

MESH = pl.DeviceIdType.MESH
def gathered_plan(integrals, amplitudes, residual_in, tile_irrep):
    tile_dev = integrals.shape[0]
    first_tile = (lax.axis_index("tile") * lax.axis_size("bulk") + lax.axis_index("bulk")) * tile_dev
    local_irrep = lax.dynamic_slice_in_dim(tile_irrep, first_tile, tile_dev, 0)
    whole_cd = lax.all_gather(amplitudes, "bulk", axis=1, tiled=True)
    picked = jnp.take(lax.all_gather(whole_cd, "tile", axis=2, tiled=True), local_irrep, axis=0)
    product = jnp.einsum("trc,tcp->trp", integrals, picked, preferred_element_type=jnp.float32)
    return (residual_in.astype(jnp.float32) + product).astype(jnp.bfloat16)


VMEM_LIMIT = 32 << 20
PLANES = 4


def kernel(rows, slots, parts, irrep_hbm, amp_hbm, int_hbm, res_hbm, out_ref, flag_hbm, *scratch):
    cols = rows // 2
    bulk = PLANES
    irrep_ref, flag, amp, ints, res, lhs, total = scratch[:7]
    scratch = scratch[7:]
    gathered, scratch = [scratch[:bulk], scratch[bulk:2 * bulk]], scratch[2 * bulk:]
    units = [1] + [parts] * (bulk - 1)
    held, picked = [None], []
    for q in range(1, bulk):
        held.append(scratch[:parts])
        scratch = scratch[parts:]
    for q in range(bulk):
        picked.append(scratch[:units[q]])
        scratch = scratch[units[q]:]
    z_send, z_recv, c_send, c_recv, p_send, p_recv, local_sem = scratch
    tiles = ints.shape[0]
    depth, width = amp.shape[1:]
    piece = depth // parts
    me, at = lax.axis_index("tile"), lax.axis_index("bulk")
    col, core = me // 2, me % 2
    partner = col * 2 + (1 - core)
    lower = at < bulk // 2
    inner = jnp.logical_and(at > 0, at < bulk - 1)
    end = jnp.where(lower, 0, bulk - 1)
    beside = jnp.where(inner, end, jnp.where(lower, 1, bulk - 2))
    across_middle = bulk - 1 - at

    first, second = inner.astype(jnp.int32), 1 - inner.astype(jnp.int32)
    plane = [jnp.where(lower, p, bulk - 1 - p) for p in (first, second, 2, 3)]

    irrep_copy = pltpu.make_async_copy(irrep_hbm, irrep_ref, local_sem.at[0])
    amp_copy = pltpu.make_async_copy(amp_hbm, amp, local_sem.at[1])
    int_copy = pltpu.make_async_copy(int_hbm, ints, local_sem.at[2])
    res_copy = pltpu.make_async_copy(res_hbm, res, local_sem.at[3])
    flag_copy = pltpu.make_async_copy(flag, flag_hbm, local_sem.at[4])
    amp_copy.start()
    irrep_copy.start()

    barrier = pltpu.get_barrier_semaphore()
    pl.semaphore_signal(barrier, inc=1, device_id=(partner, at), device_id_type=MESH)
    pl.semaphore_signal(barrier, inc=1, device_id=(me, beside), device_id_type=MESH)
    for j in range(1, cols):
        pl.semaphore_signal(barrier, inc=1, device_id=(lax.rem(col + j, cols) * 2 + core, at), device_id_type=MESH)

    @pl.when(inner)
    def _():
        pl.semaphore_signal(barrier, inc=1, device_id=(me, across_middle), device_id_type=MESH)

    int_copy.start()
    res_copy.start()
    pl.semaphore_wait(barrier, cols + 1 + first)
    amp_copy.wait()

    def band(p):
        return pl.ds(p * piece, piece)

    def line(way, p):
        src_q, dst_q = ((0, 1), (0, 2), (1, 3), (2, 2), (3, 3))[way]
        there = across_middle if way in (1, 2) else beside
        return pltpu.make_async_remote_copy(
            src_ref=amp.at[:, band(p), :] if src_q == 0 else held[src_q][p], dst_ref=held[dst_q][p],
            send_sem=z_send.at[way, p], recv_sem=z_recv.at[dst_q, p], device_id=(me, there), device_id_type=MESH)

    def line_in(q, p):
        pltpu.make_async_remote_copy(
            src_ref=held[q][p], dst_ref=held[q][p], send_sem=z_send.at[0, p],
            recv_sem=z_recv.at[q, p], device_id=(partner, at), device_id_type=MESH).wait_recv()

    def relay(q, p):
        @pl.when(inner)
        def _():
            line(q + 1, p).start()

    def rows_of(q, u):
        return pl.ds(0, depth) if units[q] == 1 else band(u)

    def slab(side, q, u, column):
        return gathered[side][q].at[:, rows_of(q, u), pl.ds(pl.multiple_of(column * width, 128), width)]

    def across(q, u, j):
        return pltpu.make_async_remote_copy(
            src_ref=picked[q][u].at[j - 1], dst_ref=slab(0, q, u, col), send_sem=c_send.at[q, u, j],
            recv_sem=c_recv.at[q, u, j], device_id=(lax.rem(col + j, cols) * 2 + core, at), device_id_type=MESH)

    def over(q, u, j):
        column = lax.rem(col - j + cols, cols)
        return pltpu.make_async_remote_copy(
            src_ref=slab(0, q, u, column), dst_ref=slab(1, q, u, column), send_sem=p_send.at[q, u, j],
            recv_sem=p_recv.at[q, u, j], device_id=(partner, at), device_id_type=MESH)

    def wanted(column):
        low = (2 * column * bulk + at) * tiles
        high = ((2 * column + 1) * bulk + at) * tiles + tiles - 1
        spots = [low, high] if slots == 2 else [low, low + tiles - 1, high]
        return [irrep_ref[s] for s in spots]

    def spread(q, u):
        src = amp if q == 0 else held[q][u]
        for k in range(1, cols):
            j = lax.rem(k - 1 + (k > col).astype(jnp.int32) - col + cols, cols)
            for s, g in enumerate(wanted(lax.rem(col + j, cols))):
                picked[q][u][j - 1, s] = src[g]
            across(q, u, j).start()
        for s, g in enumerate(mine):
            gathered[0][q][s, rows_of(q, u), pl.ds(pl.multiple_of(col * width, 128), width)] = src[g]
        over(q, u, 0).start()

    def forward(q):
        for u in range(units[q]):
            for j in range(1, cols):
                landed = slab(0, q, u, lax.rem(col - j + cols, cols))
                pltpu.make_async_remote_copy(
                    src_ref=landed, dst_ref=landed, send_sem=c_send.at[q, u, j], recv_sem=c_recv.at[q, u, j],
                    device_id=(partner, at), device_id_type=MESH).wait_recv()
                over(q, u, j).start()

    first_tile = (me * bulk + at) * tiles

    def product(q, side):
        for t in range(tiles):
            irrep = irrep_ref[first_tile + t]
            slot = (irrep > mine[0]).astype(jnp.int32)
            for s in mine[1:-1]:
                slot = slot + (irrep > s).astype(jnp.int32)
            part = jnp.dot(lhs[plane[q], t], gathered[side][q][slot], preferred_element_type=jnp.float32)
            if q > 0:
                part = part + total[side, t]
            if 0 < q < bulk - 1:
                total[side, t] = part
                continue
            for n in range(cols):
                there = pl.ds(pl.multiple_of((n * 2 + (core if side == 0 else 1 - core)) * width, width), width)
                here = part[:, n * width:(n + 1) * width]
                if q > 0:
                    out_ref[t, :, there] = here.astype(jnp.bfloat16)
                else:
                    total[side, t, :, n * width:(n + 1) * width] = here + res[t, :, there].astype(jnp.float32)

    def arrived(q):
        for u in range(units[q]):
            for j in range(cols):
                over(q, u, j).wait_recv()

    def add(q):
        arrived(q)
        for side in range(2):
            product(q, side)

    for p in range(parts):
        line(0, p).start()

        @pl.when(inner)
        def _():
            line(1, p).start()

    irrep_copy.wait()
    mine = wanted(col)
    spread(0, 0)
    third = jnp.int32(0)
    for column in range(cols):
        for level in range(bulk):
            low = irrep_ref[(2 * column * bulk + level) * tiles]
            high = irrep_ref[((2 * column + 1) * bulk + level) * tiles + tiles - 1]
            third = third + (high > low + 1).astype(jnp.int32)
    flag[0] = third
    flag_copy.start()
    int_copy.wait()
    for k in range(bulk):
        for t in range(tiles):
            lhs[k, t] = ints[t, :, k * depth:(k + 1) * depth]
    res_copy.wait()
    flag_copy.wait()

    for p in range(parts):
        line_in(1, p)
        relay(1, p)
        spread(1, p)
        if p < parts - 1:
            @pl.when(inner)
            def _():
                line_in(2, p)
                line(3, p).start()
    for p in range(parts):
        if p < parts - 1:
            @pl.when(jnp.logical_not(inner))
            def _():
                line_in(2, p)
        else:
            line_in(2, p)
            relay(2, p)
        spread(2, p)
    forward(0)
    for p in range(parts):
        line_in(3, p)
        relay(3, p)
        spread(3, p)
    add(0)
    forward(1)
    add(1)
    forward(2)
    add(2)
    forward(3)
    product(3, 0)
    arrived(3)
    product(3, 1)

    for q in range(bulk):
        for u in range(units[q]):
            for j in range(cols):
                over(q, u, j).wait_send()
            for j in range(1, cols):
                across(q, u, j).wait_send()
    for p in range(parts):
        line(0, p).wait_send()

        @pl.when(inner)
        def _():
            for way in range(1, 5):
                line(way, p).wait_send()


def call(rows, slots, integrals, amplitudes, residual_in, tile_irrep):
    irreps, depth, width = amplitudes.shape
    tiles, height = integrals.shape[:2]
    parts = 2 if depth % 32 == 0 else 1
    bulk = PLANES
    cols = rows // 2
    hbm = pl.BlockSpec(memory_space=pltpu.HBM)
    kind = amplitudes.dtype
    picked = [depth] + [depth // parts] * (parts * (bulk - 1))
    return pl.pallas_call(
        functools.partial(kernel, rows, slots, parts),
        out_shape=(
            jax.ShapeDtypeStruct(residual_in.shape, residual_in.dtype),
            jax.ShapeDtypeStruct((1,), jnp.int32),
        ),
        in_specs=[hbm] * 4,
        out_specs=(pl.BlockSpec(memory_space=pltpu.VMEM), hbm),
        scratch_shapes=[
            pltpu.SMEM(tile_irrep.shape, tile_irrep.dtype),
            pltpu.SMEM((1,), jnp.int32),
            pltpu.VMEM(amplitudes.shape, kind),
            pltpu.VMEM(integrals.shape, integrals.dtype),
            pltpu.VMEM(residual_in.shape, residual_in.dtype),
            pltpu.VMEM((bulk, tiles, height, depth), integrals.dtype),
            pltpu.VMEM((2, tiles, height, cols * width), jnp.float32),
            *[pltpu.VMEM((slots, depth, cols * width), kind)] * (2 * bulk),
            *[pltpu.VMEM((irreps, depth // parts, width), kind)] * (parts * (bulk - 1)),
            *[pltpu.VMEM((cols - 1, slots, size, width), kind) for size in picked],
            pltpu.SemaphoreType.DMA((5, parts)),
            pltpu.SemaphoreType.DMA((bulk, parts)),
            *[pltpu.SemaphoreType.DMA((bulk, parts, cols))] * 4,
            pltpu.SemaphoreType.DMA((5,)),
        ],
        compiler_params=pltpu.CompilerParams(collective_id=slots, has_side_effects=True, vmem_limit_bytes=VMEM_LIMIT),
    )(tile_irrep, amplitudes, integrals, residual_in)


def local(rows, bulk, integrals, amplitudes, residual_in, tile_irrep):
    depth, width = amplitudes.shape[1:]
    if rows % 2 or rows < 4 or bulk != PLANES or depth % 16 or width % 128:
        return gathered_plan(integrals, amplitudes, residual_in, tile_irrep)
    out, third = call(rows, 2, integrals, amplitudes, residual_in, tile_irrep)
    return lax.cond(
        third[0] > 0,
        lambda out, *args: call(rows, 3, *[pltpu.with_memory_space_constraint(x, pltpu.HBM) for x in args])[0],
        lambda out, *args: out,
        out, integrals, amplitudes, residual_in, tile_irrep)


def solution(mesh):
    return jax.shard_map(
        functools.partial(local, mesh.shape["tile"], mesh.shape["bulk"]),
        mesh=mesh,
        in_specs=(
            P(("tile", "bulk"), None, None),
            P(None, "bulk", "tile"),
            P(("tile", "bulk"), None, None),
            P(),
        ),
        out_specs=P(("tile", "bulk"), None, None),
        check_vma=False,
    )
```

```python
import functools

import jax
import jax.numpy as jnp
from jax import lax
from jax.experimental import pallas as pl
from jax.experimental.pallas import tpu as pltpu
from jax.sharding import PartitionSpec as P

MESH = pl.DeviceIdType.MESH
def gathered_plan(integrals, amplitudes, residual_in, tile_irrep):
    tile_dev = integrals.shape[0]
    first_tile = (lax.axis_index("tile") * lax.axis_size("bulk") + lax.axis_index("bulk")) * tile_dev
    local_irrep = lax.dynamic_slice_in_dim(tile_irrep, first_tile, tile_dev, 0)
    whole_cd = lax.all_gather(amplitudes, "bulk", axis=1, tiled=True)
    picked = jnp.take(lax.all_gather(whole_cd, "tile", axis=2, tiled=True), local_irrep, axis=0)
    product = jnp.einsum("trc,tcp->trp", integrals, picked, preferred_element_type=jnp.float32)
    return (residual_in.astype(jnp.float32) + product).astype(jnp.bfloat16)


VMEM_LIMIT = 32 << 20
PLANES = 4


def kernel(rows, slots, parts, irrep_hbm, amp_hbm, int_hbm, res_hbm, out_ref, flag_hbm, *scratch):
    cols = rows // 2
    bulk = PLANES
    irrep_ref, flag, amp, ints, res, lhs, total = scratch[:7]
    scratch = scratch[7:]
    gathered, scratch = [scratch[:bulk], scratch[bulk:2 * bulk]], scratch[2 * bulk:]
    units = [1] + [parts] * (bulk - 1)
    held, picked = [None], []
    for q in range(1, bulk):
        held.append(scratch[:parts])
        scratch = scratch[parts:]
    for q in range(bulk):
        picked.append(scratch[:units[q]])
        scratch = scratch[units[q]:]
    z_send, z_recv, c_send, c_recv, p_send, p_recv, local_sem = scratch
    tiles = ints.shape[0]
    depth, width = amp.shape[1:]
    piece = depth // parts
    me, at = lax.axis_index("tile"), lax.axis_index("bulk")
    col, core = me // 2, me % 2
    partner = col * 2 + (1 - core)
    lower = at < bulk // 2
    inner = jnp.logical_and(at > 0, at < bulk - 1)
    end = jnp.where(lower, 0, bulk - 1)
    beside = jnp.where(inner, end, jnp.where(lower, 1, bulk - 2))
    across_middle = bulk - 1 - at

    first, second = inner.astype(jnp.int32), 1 - inner.astype(jnp.int32)
    plane = [jnp.where(lower, p, bulk - 1 - p) for p in (first, second, 2, 3)]

    irrep_copy = pltpu.make_async_copy(irrep_hbm, irrep_ref, local_sem.at[0])
    amp_copy = pltpu.make_async_copy(amp_hbm, amp, local_sem.at[1])
    int_copy = pltpu.make_async_copy(int_hbm, ints, local_sem.at[2])
    res_copy = pltpu.make_async_copy(res_hbm, res, local_sem.at[3])
    flag_copy = pltpu.make_async_copy(flag, flag_hbm, local_sem.at[4])
    amp_copy.start()
    irrep_copy.start()

    barrier = pltpu.get_barrier_semaphore()
    pl.semaphore_signal(barrier, inc=1, device_id=(partner, at), device_id_type=MESH)
    pl.semaphore_signal(barrier, inc=1, device_id=(me, beside), device_id_type=MESH)
    for j in range(1, cols):
        pl.semaphore_signal(barrier, inc=1, device_id=(lax.rem(col + j, cols) * 2 + core, at), device_id_type=MESH)

    @pl.when(inner)
    def _():
        pl.semaphore_signal(barrier, inc=1, device_id=(me, across_middle), device_id_type=MESH)

    int_copy.start()
    res_copy.start()
    pl.semaphore_wait(barrier, cols + 1 + first)
    amp_copy.wait()

    def band(p):
        return pl.ds(p * piece, piece)

    def line(way, p):
        src_q, dst_q = ((0, 1), (0, 2), (1, 3), (2, 2), (3, 3))[way]
        there = across_middle if way in (1, 2) else beside
        return pltpu.make_async_remote_copy(
            src_ref=amp.at[:, band(p), :] if src_q == 0 else held[src_q][p], dst_ref=held[dst_q][p],
            send_sem=z_send.at[way, p], recv_sem=z_recv.at[dst_q, p], device_id=(me, there), device_id_type=MESH)

    def line_in(q, p):
        pltpu.make_async_remote_copy(
            src_ref=held[q][p], dst_ref=held[q][p], send_sem=z_send.at[0, p],
            recv_sem=z_recv.at[q, p], device_id=(partner, at), device_id_type=MESH).wait_recv()

    def rows_of(q, u):
        return pl.ds(0, depth) if units[q] == 1 else band(u)

    def slab(side, q, u, column):
        return gathered[side][q].at[:, rows_of(q, u), pl.ds(pl.multiple_of(column * width, 128), width)]

    def across(q, u, j):
        return pltpu.make_async_remote_copy(
            src_ref=picked[q][u].at[j - 1], dst_ref=slab(0, q, u, col), send_sem=c_send.at[q, u, j],
            recv_sem=c_recv.at[q, u, j], device_id=(lax.rem(col + j, cols) * 2 + core, at), device_id_type=MESH)

    def over(q, u, j):
        column = lax.rem(col - j + cols, cols)
        return pltpu.make_async_remote_copy(
            src_ref=slab(0, q, u, column), dst_ref=slab(1, q, u, column), send_sem=p_send.at[q, u, j],
            recv_sem=p_recv.at[q, u, j], device_id=(partner, at), device_id_type=MESH)

    def wanted(column):
        low = (2 * column * bulk + at) * tiles
        high = ((2 * column + 1) * bulk + at) * tiles + tiles - 1
        spots = [low, high] if slots == 2 else [low, low + tiles - 1, high]
        return [irrep_ref[s] for s in spots]

    def spread(q, u):
        src = amp if q == 0 else held[q][u]
        for k in range(1, cols):
            j = lax.rem(k - 1 + (k > col).astype(jnp.int32) - col + cols, cols)
            for s, g in enumerate(wanted(lax.rem(col + j, cols))):
                picked[q][u][j - 1, s] = src[g]
            across(q, u, j).start()
        for s, g in enumerate(mine):
            gathered[0][q][s, rows_of(q, u), pl.ds(pl.multiple_of(col * width, 128), width)] = src[g]
        over(q, u, 0).start()

    def forward(q):
        for u in range(units[q]):
            for j in range(1, cols):
                landed = slab(0, q, u, lax.rem(col - j + cols, cols))
                pltpu.make_async_remote_copy(
                    src_ref=landed, dst_ref=landed, send_sem=c_send.at[q, u, j], recv_sem=c_recv.at[q, u, j],
                    device_id=(partner, at), device_id_type=MESH).wait_recv()
                over(q, u, j).start()

    first_tile = (me * bulk + at) * tiles

    def product(q, side):
        for t in range(tiles):
            irrep = irrep_ref[first_tile + t]
            slot = (irrep > mine[0]).astype(jnp.int32)
            for s in mine[1:-1]:
                slot = slot + (irrep > s).astype(jnp.int32)
            part = jnp.dot(lhs[plane[q], t], gathered[side][q][slot], preferred_element_type=jnp.float32)
            if q > 0:
                part = part + total[side, t]
            if 0 < q < bulk - 1:
                total[side, t] = part
                continue
            for n in range(cols):
                there = pl.ds(pl.multiple_of((n * 2 + (core if side == 0 else 1 - core)) * width, width), width)
                here = part[:, n * width:(n + 1) * width]
                if q > 0:
                    out_ref[t, :, there] = here.astype(jnp.bfloat16)
                else:
                    total[side, t, :, n * width:(n + 1) * width] = here + res[t, :, there].astype(jnp.float32)

    def arrived(q):
        for u in range(units[q]):
            for j in range(cols):
                over(q, u, j).wait_recv()

    def add(q):
        arrived(q)
        for side in range(2):
            product(q, side)

    for p in range(parts):
        line(0, p).start()

        @pl.when(inner)
        def _():
            line(1, p).start()

    irrep_copy.wait()
    mine = wanted(col)
    spread(0, 0)
    third = jnp.int32(0)
    for column in range(cols):
        for level in range(bulk):
            low = irrep_ref[(2 * column * bulk + level) * tiles]
            high = irrep_ref[((2 * column + 1) * bulk + level) * tiles + tiles - 1]
            third = third + (high > low + 1).astype(jnp.int32)
    flag[0] = third
    flag_copy.start()
    int_copy.wait()
    for k in range(bulk):
        for t in range(tiles):
            lhs[k, t] = ints[t, :, k * depth:(k + 1) * depth]
    res_copy.wait()
    flag_copy.wait()

    for p in range(parts):
        line_in(1, p)

        @pl.when(inner)
        def _():
            line(2, p).start()
            line_in(2, p)
            line(3, p).start()

        spread(1, p)
    for p in range(parts):
        @pl.when(jnp.logical_not(inner))
        def _():
            line_in(2, p)

        spread(2, p)
    @pl.when(inner)
    def _():
        for p in range(parts):
            line_in(3, p)
            line(4, p).start()

    forward(0)
    for p in range(parts):
        @pl.when(jnp.logical_not(inner))
        def _():
            line_in(3, p)

        spread(3, p)
    forward(1)
    add(0)
    forward(2)
    add(1)
    add(2)
    forward(3)
    product(3, 0)
    arrived(3)
    product(3, 1)

    for q in range(bulk):
        for u in range(units[q]):
            for j in range(cols):
                over(q, u, j).wait_send()
            for j in range(1, cols):
                across(q, u, j).wait_send()
    for p in range(parts):
        line(0, p).wait_send()

        @pl.when(inner)
        def _():
            for way in range(1, 5):
                line(way, p).wait_send()


def call(rows, slots, integrals, amplitudes, residual_in, tile_irrep):
    irreps, depth, width = amplitudes.shape
    tiles, height = integrals.shape[:2]
    parts = 2 if depth % 32 == 0 else 1
    bulk = PLANES
    cols = rows // 2
    hbm = pl.BlockSpec(memory_space=pltpu.HBM)
    kind = amplitudes.dtype
    picked = [depth] + [depth // parts] * (parts * (bulk - 1))
    return pl.pallas_call(
        functools.partial(kernel, rows, slots, parts),
        out_shape=(
            jax.ShapeDtypeStruct(residual_in.shape, residual_in.dtype),
            jax.ShapeDtypeStruct((1,), jnp.int32),
        ),
        in_specs=[hbm] * 4,
        out_specs=(pl.BlockSpec(memory_space=pltpu.VMEM), hbm),
        scratch_shapes=[
            pltpu.SMEM(tile_irrep.shape, tile_irrep.dtype),
            pltpu.SMEM((1,), jnp.int32),
            pltpu.VMEM(amplitudes.shape, kind),
            pltpu.VMEM(integrals.shape, integrals.dtype),
            pltpu.VMEM(residual_in.shape, residual_in.dtype),
            pltpu.VMEM((bulk, tiles, height, depth), integrals.dtype),
            pltpu.VMEM((2, tiles, height, cols * width), jnp.float32),
            *[pltpu.VMEM((slots, depth, cols * width), kind)] * (2 * bulk),
            *[pltpu.VMEM((irreps, depth // parts, width), kind)] * (parts * (bulk - 1)),
            *[pltpu.VMEM((cols - 1, slots, size, width), kind) for size in picked],
            pltpu.SemaphoreType.DMA((5, parts)),
            pltpu.SemaphoreType.DMA((bulk, parts)),
            *[pltpu.SemaphoreType.DMA((bulk, parts, cols))] * 4,
            pltpu.SemaphoreType.DMA((5,)),
        ],
        compiler_params=pltpu.CompilerParams(collective_id=slots, has_side_effects=True, vmem_limit_bytes=VMEM_LIMIT),
    )(tile_irrep, amplitudes, integrals, residual_in)


def local(rows, bulk, integrals, amplitudes, residual_in, tile_irrep):
    depth, width = amplitudes.shape[1:]
    if rows % 2 or rows < 4 or bulk != PLANES or depth % 16 or width % 128:
        return gathered_plan(integrals, amplitudes, residual_in, tile_irrep)
    out, third = call(rows, 2, integrals, amplitudes, residual_in, tile_irrep)
    return lax.cond(
        third[0] > 0,
        lambda out, *args: call(rows, 3, *[pltpu.with_memory_space_constraint(x, pltpu.HBM) for x in args])[0],
        lambda out, *args: out,
        out, integrals, amplitudes, residual_in, tile_irrep)


def solution(mesh):
    return jax.shard_map(
        functools.partial(local, mesh.shape["tile"], mesh.shape["bulk"]),
        mesh=mesh,
        in_specs=(
            P(("tile", "bulk"), None, None),
            P(None, "bulk", "tile"),
            P(("tile", "bulk"), None, None),
            P(),
        ),
        out_specs=P(("tile", "bulk"), None, None),
        check_vma=False,
    )
```

```python
import functools

import jax
import jax.numpy as jnp
from jax import lax
from jax.experimental import pallas as pl
from jax.experimental.pallas import tpu as pltpu
from jax.sharding import PartitionSpec as P

MESH = pl.DeviceIdType.MESH
def gathered_plan(integrals, amplitudes, residual_in, tile_irrep):
    tile_dev = integrals.shape[0]
    first_tile = (lax.axis_index("tile") * lax.axis_size("bulk") + lax.axis_index("bulk")) * tile_dev
    local_irrep = lax.dynamic_slice_in_dim(tile_irrep, first_tile, tile_dev, 0)
    whole_cd = lax.all_gather(amplitudes, "bulk", axis=1, tiled=True)
    picked = jnp.take(lax.all_gather(whole_cd, "tile", axis=2, tiled=True), local_irrep, axis=0)
    product = jnp.einsum("trc,tcp->trp", integrals, picked, preferred_element_type=jnp.float32)
    return (residual_in.astype(jnp.float32) + product).astype(jnp.bfloat16)


VMEM_LIMIT = 32 << 20
PLANES = 4
COLUMNS = 4


def kernel(rows, slots, parts, irrep_hbm, amp_hbm, int_hbm, res_hbm, out_ref, flag_hbm, *scratch):
    cols = rows // 2
    bulk = PLANES
    irrep_ref, flag, amp, ints, res, lhs, total = scratch[:7]
    scratch = scratch[7:]
    gathered, scratch = [scratch[:bulk], scratch[bulk:2 * bulk]], scratch[2 * bulk:]
    units = [1] + [parts] * (bulk - 1)
    held, picked = [None], []
    for q in range(1, bulk):
        held.append(scratch[:parts])
        scratch = scratch[parts:]
    for q in range(bulk):
        picked.append(scratch[:units[q]])
        scratch = scratch[units[q]:]
    z_send, z_recv, c_send, c_recv, p_send, p_recv, local_sem, vouched = scratch
    tiles = ints.shape[0]
    depth, width = amp.shape[1:]
    piece = depth // parts
    me, at = lax.axis_index("tile"), lax.axis_index("bulk")
    col, core = me // 2, me % 2
    partner = col * 2 + (1 - core)
    lower = at < bulk // 2
    inner = jnp.logical_and(at > 0, at < bulk - 1)
    end = jnp.where(lower, 0, bulk - 1)
    beside = jnp.where(inner, end, jnp.where(lower, 1, bulk - 2))
    across_middle = bulk - 1 - at

    first, second = inner.astype(jnp.int32), 1 - inner.astype(jnp.int32)
    plane = [jnp.where(lower, p, bulk - 1 - p) for p in (first, second, 2, 3)]

    irrep_copy = pltpu.make_async_copy(irrep_hbm, irrep_ref, local_sem.at[0])
    amp_copy = pltpu.make_async_copy(amp_hbm, amp, local_sem.at[1])
    int_copy = pltpu.make_async_copy(int_hbm, ints, local_sem.at[2])
    res_copy = pltpu.make_async_copy(res_hbm, res, local_sem.at[3])
    flag_copy = pltpu.make_async_copy(flag, flag_hbm, local_sem.at[4])
    amp_copy.start()
    irrep_copy.start()

    odd, half = col % 2, col // 2
    near = [half * 2 + 1 - odd, (1 - half) * 2 + odd]
    far = (1 - half) * 2 + 1 - odd

    barrier = pltpu.get_barrier_semaphore()
    pl.semaphore_signal(barrier, inc=1, device_id=(partner, at), device_id_type=MESH)
    pl.semaphore_signal(barrier, inc=1, device_id=(me, beside), device_id_type=MESH)
    for column in near:
        pl.semaphore_signal(barrier, inc=1, device_id=(column * 2 + core, at), device_id_type=MESH)

    @pl.when(inner)
    def _():
        pl.semaphore_signal(barrier, inc=1, device_id=(me, across_middle), device_id_type=MESH)

    int_copy.start()
    res_copy.start()
    pl.semaphore_wait(barrier, 2 + len(near) + first)
    pl.semaphore_signal(vouched, inc=1, device_id=(near[0] * 2 + core, at), device_id_type=MESH)
    amp_copy.wait()

    def band(p):
        return pl.ds(p * piece, piece)

    def line(way, p):
        src_q, dst_q = ((0, 1), (0, 2), (1, 3), (2, 2), (3, 3))[way]
        there = across_middle if way in (1, 2) else beside
        return pltpu.make_async_remote_copy(
            src_ref=amp.at[:, band(p), :] if src_q == 0 else held[src_q][p], dst_ref=held[dst_q][p],
            send_sem=z_send.at[way, p], recv_sem=z_recv.at[dst_q, p], device_id=(me, there), device_id_type=MESH)

    def line_in(q, p):
        pltpu.make_async_remote_copy(
            src_ref=held[q][p], dst_ref=held[q][p], send_sem=z_send.at[0, p],
            recv_sem=z_recv.at[q, p], device_id=(partner, at), device_id_type=MESH).wait_recv()

    def rows_of(q, u):
        return pl.ds(0, depth) if units[q] == 1 else band(u)

    def slab(side, q, u, column):
        return gathered[side][q].at[:, rows_of(q, u), pl.ds(pl.multiple_of(column * width, 128), width)]

    def across(q, u, j):
        return pltpu.make_async_remote_copy(
            src_ref=picked[q][u].at[j - 1], dst_ref=slab(0, q, u, col), send_sem=c_send.at[q, u, j],
            recv_sem=c_recv.at[q, u, j], device_id=(lax.rem(col + j, cols) * 2 + core, at), device_id_type=MESH)

    def over(q, u, j):
        column = lax.rem(col - j + cols, cols)
        return pltpu.make_async_remote_copy(
            src_ref=slab(0, q, u, column), dst_ref=slab(1, q, u, column), send_sem=p_send.at[q, u, j],
            recv_sem=p_recv.at[q, u, j], device_id=(partner, at), device_id_type=MESH)

    def wanted(column):
        low = (2 * column * bulk + at) * tiles
        high = ((2 * column + 1) * bulk + at) * tiles + tiles - 1
        spots = [low, high] if slots == 2 else [low, low + tiles - 1, high]
        return [irrep_ref[s] for s in spots]

    def spread(q, u):
        src = amp if q == 0 else held[q][u]
        rising = [k + (k >= col).astype(jnp.int32) for k in range(cols - 1)]
        for column in (near[1], near[0], far) if q == 0 else rising:
            j = lax.rem(column - col + cols, cols)
            for s, g in enumerate(wanted(lax.rem(col + j, cols))):
                picked[q][u][j - 1, s] = src[g]
            if q == 0 and column is far:
                pl.semaphore_wait(vouched, 1)
            across(q, u, j).start()
        for s, g in enumerate(mine):
            gathered[0][q][s, rows_of(q, u), pl.ds(pl.multiple_of(col * width, 128), width)] = src[g]
        over(q, u, 0).start()

    def forward(q):
        for u in range(units[q]):
            for column in (*near, far):
                j = lax.rem(col - column + cols, cols)
                landed = slab(0, q, u, column)
                pltpu.make_async_remote_copy(
                    src_ref=landed, dst_ref=landed, send_sem=c_send.at[q, u, j], recv_sem=c_recv.at[q, u, j],
                    device_id=(partner, at), device_id_type=MESH).wait_recv()
                over(q, u, j).start()

    first_tile = (me * bulk + at) * tiles

    def product(q, side):
        for t in range(tiles):
            irrep = irrep_ref[first_tile + t]
            slot = (irrep > mine[0]).astype(jnp.int32)
            for s in mine[1:-1]:
                slot = slot + (irrep > s).astype(jnp.int32)
            part = jnp.dot(lhs[plane[q], t], gathered[side][q][slot], preferred_element_type=jnp.float32)
            if q > 0:
                part = part + total[side, t]
            if 0 < q < bulk - 1:
                total[side, t] = part
                continue
            for n in range(cols):
                there = pl.ds(pl.multiple_of((n * 2 + (core if side == 0 else 1 - core)) * width, width), width)
                here = part[:, n * width:(n + 1) * width]
                if q > 0:
                    out_ref[t, :, there] = here.astype(jnp.bfloat16)
                else:
                    total[side, t, :, n * width:(n + 1) * width] = here + res[t, :, there].astype(jnp.float32)

    def arrived(q):
        for u in range(units[q]):
            for j in range(cols):
                over(q, u, j).wait_recv()

    def add(q):
        arrived(q)
        for side in range(2):
            product(q, side)

    for p in range(parts):
        line(0, p).start()

        @pl.when(inner)
        def _():
            line(1, p).start()

    irrep_copy.wait()
    mine = wanted(col)
    spread(0, 0)
    third = jnp.int32(0)
    for column in range(cols):
        for level in range(bulk):
            low = irrep_ref[(2 * column * bulk + level) * tiles]
            high = irrep_ref[((2 * column + 1) * bulk + level) * tiles + tiles - 1]
            third = third + (high > low + 1).astype(jnp.int32)
    flag[0] = third
    flag_copy.start()
    int_copy.wait()
    for k in range(bulk):
        for t in range(tiles):
            lhs[k, t] = ints[t, :, k * depth:(k + 1) * depth]
    res_copy.wait()
    flag_copy.wait()

    for p in range(parts):
        line_in(1, p)

        @pl.when(inner)
        def _():
            line(2, p).start()
            line_in(2, p)
            line(3, p).start()

        spread(1, p)
    for p in range(parts):
        @pl.when(jnp.logical_not(inner))
        def _():
            line_in(2, p)

        spread(2, p)
    @pl.when(inner)
    def _():
        for p in range(parts):
            line_in(3, p)
            line(4, p).start()

    forward(0)
    for p in range(parts):
        @pl.when(jnp.logical_not(inner))
        def _():
            line_in(3, p)

        spread(3, p)
    forward(1)
    add(0)
    forward(2)
    add(1)
    add(2)
    forward(3)
    product(3, 0)
    arrived(3)
    product(3, 1)

    for q in range(bulk):
        for u in range(units[q]):
            for j in range(cols):
                over(q, u, j).wait_send()
            for j in range(1, cols):
                across(q, u, j).wait_send()
    for p in range(parts):
        line(0, p).wait_send()

        @pl.when(inner)
        def _():
            for way in range(1, 5):
                line(way, p).wait_send()


def call(rows, slots, integrals, amplitudes, residual_in, tile_irrep):
    irreps, depth, width = amplitudes.shape
    tiles, height = integrals.shape[:2]
    parts = 2 if depth % 32 == 0 else 1
    bulk = PLANES
    cols = rows // 2
    hbm = pl.BlockSpec(memory_space=pltpu.HBM)
    kind = amplitudes.dtype
    picked = [depth] + [depth // parts] * (parts * (bulk - 1))
    return pl.pallas_call(
        functools.partial(kernel, rows, slots, parts),
        out_shape=(
            jax.ShapeDtypeStruct(residual_in.shape, residual_in.dtype),
            jax.ShapeDtypeStruct((1,), jnp.int32),
        ),
        in_specs=[hbm] * 4,
        out_specs=(pl.BlockSpec(memory_space=pltpu.VMEM), hbm),
        scratch_shapes=[
            pltpu.SMEM(tile_irrep.shape, tile_irrep.dtype),
            pltpu.SMEM((1,), jnp.int32),
            pltpu.VMEM(amplitudes.shape, kind),
            pltpu.VMEM(integrals.shape, integrals.dtype),
            pltpu.VMEM(residual_in.shape, residual_in.dtype),
            pltpu.VMEM((bulk, tiles, height, depth), integrals.dtype),
            pltpu.VMEM((2, tiles, height, cols * width), jnp.float32),
            *[pltpu.VMEM((slots, depth, cols * width), kind)] * (2 * bulk),
            *[pltpu.VMEM((irreps, depth // parts, width), kind)] * (parts * (bulk - 1)),
            *[pltpu.VMEM((cols - 1, slots, size, width), kind) for size in picked],
            pltpu.SemaphoreType.DMA((5, parts)),
            pltpu.SemaphoreType.DMA((bulk, parts)),
            *[pltpu.SemaphoreType.DMA((bulk, parts, cols))] * 4,
            pltpu.SemaphoreType.DMA((5,)),
            pltpu.SemaphoreType.REGULAR,
        ],
        compiler_params=pltpu.CompilerParams(collective_id=slots, has_side_effects=True, vmem_limit_bytes=VMEM_LIMIT),
    )(tile_irrep, amplitudes, integrals, residual_in)


def local(rows, bulk, integrals, amplitudes, residual_in, tile_irrep):
    depth, width = amplitudes.shape[1:]
    if rows != 2 * COLUMNS or bulk != PLANES or depth % 16 or width % 128:
        return gathered_plan(integrals, amplitudes, residual_in, tile_irrep)
    out, third = call(rows, 2, integrals, amplitudes, residual_in, tile_irrep)
    return lax.cond(
        third[0] > 0,
        lambda out, *args: call(rows, 3, *[pltpu.with_memory_space_constraint(x, pltpu.HBM) for x in args])[0],
        lambda out, *args: out,
        out, integrals, amplitudes, residual_in, tile_irrep)


def solution(mesh):
    return jax.shard_map(
        functools.partial(local, mesh.shape["tile"], mesh.shape["bulk"]),
        mesh=mesh,
        in_specs=(
            P(("tile", "bulk"), None, None),
            P(None, "bulk", "tile"),
            P(("tile", "bulk"), None, None),
            P(),
        ),
        out_specs=P(("tile", "bulk"), None, None),
        check_vma=False,
    )
```

```python
import functools

import jax
import jax.numpy as jnp
from jax import lax
from jax.experimental import pallas as pl
from jax.experimental.pallas import tpu as pltpu
from jax.sharding import PartitionSpec as P

MESH = pl.DeviceIdType.MESH
def gathered_plan(integrals, amplitudes, residual_in, tile_irrep):
    tile_dev = integrals.shape[0]
    first_tile = (lax.axis_index("tile") * lax.axis_size("bulk") + lax.axis_index("bulk")) * tile_dev
    local_irrep = lax.dynamic_slice_in_dim(tile_irrep, first_tile, tile_dev, 0)
    whole_cd = lax.all_gather(amplitudes, "bulk", axis=1, tiled=True)
    picked = jnp.take(lax.all_gather(whole_cd, "tile", axis=2, tiled=True), local_irrep, axis=0)
    product = jnp.einsum("trc,tcp->trp", integrals, picked, preferred_element_type=jnp.float32)
    return (residual_in.astype(jnp.float32) + product).astype(jnp.bfloat16)


VMEM_LIMIT = 32 << 20
PLANES = 4
COLUMNS = 4


def kernel(rows, slots, parts, irrep_hbm, amp_hbm, int_hbm, res_hbm, out_ref, flag_hbm, *scratch):
    cols = rows // 2
    bulk = PLANES
    irrep_ref, flag, amp, ints, res, lhs, total = scratch[:7]
    scratch = scratch[7:]
    gathered, scratch = [scratch[:bulk], scratch[bulk:2 * bulk]], scratch[2 * bulk:]
    units = [1] + [parts] * (bulk - 1)
    held, picked = [None], []
    for q in range(1, bulk):
        held.append(scratch[:parts])
        scratch = scratch[parts:]
    for q in range(bulk):
        picked.append(scratch[:units[q]])
        scratch = scratch[units[q]:]
    z_send, z_recv, c_send, c_recv, p_send, p_recv, local_sem, vouched = scratch
    tiles = ints.shape[0]
    depth, width = amp.shape[1:]
    piece = depth // parts
    me, at = lax.axis_index("tile"), lax.axis_index("bulk")
    col, core = me // 2, me % 2
    partner = col * 2 + (1 - core)
    lower = at < bulk // 2
    inner = jnp.logical_and(at > 0, at < bulk - 1)
    end = jnp.where(lower, 0, bulk - 1)
    beside = jnp.where(inner, end, jnp.where(lower, 1, bulk - 2))
    across_middle = bulk - 1 - at

    first, second = inner.astype(jnp.int32), 1 - inner.astype(jnp.int32)
    plane = [jnp.where(lower, p, bulk - 1 - p) for p in (first, second, 2, 3)]

    irrep_copy = pltpu.make_async_copy(irrep_hbm, irrep_ref, local_sem.at[0])
    amp_copy = pltpu.make_async_copy(amp_hbm, amp, local_sem.at[1])
    int_copy = pltpu.make_async_copy(int_hbm, ints, local_sem.at[2])
    res_copy = pltpu.make_async_copy(res_hbm, res, local_sem.at[3])
    flag_copy = pltpu.make_async_copy(flag, flag_hbm, local_sem.at[4])
    amp_copy.start()
    irrep_copy.start()

    odd, half = col % 2, col // 2
    near = [half * 2 + 1 - odd, (1 - half) * 2 + odd]
    far = (1 - half) * 2 + 1 - odd

    barrier = pltpu.get_barrier_semaphore()
    pl.semaphore_signal(barrier, inc=1, device_id=(partner, at), device_id_type=MESH)
    pl.semaphore_signal(barrier, inc=1, device_id=(me, beside), device_id_type=MESH)
    for column in near:
        pl.semaphore_signal(barrier, inc=1, device_id=(column * 2 + core, at), device_id_type=MESH)

    @pl.when(inner)
    def _():
        pl.semaphore_signal(barrier, inc=1, device_id=(me, across_middle), device_id_type=MESH)

    int_copy.start()
    res_copy.start()
    pl.semaphore_wait(barrier, 2 + len(near) + first)
    pl.semaphore_signal(vouched, inc=1, device_id=(near[0] * 2 + core, at), device_id_type=MESH)
    amp_copy.wait()

    def band(p):
        return pl.ds(p * piece, piece)

    def line(way, p):
        src_q, dst_q = ((0, 1), (0, 2), (1, 3), (2, 2), (3, 3))[way]
        there = across_middle if way in (1, 2) else beside
        return pltpu.make_async_remote_copy(
            src_ref=amp.at[:, band(p), :] if src_q == 0 else held[src_q][p], dst_ref=held[dst_q][p],
            send_sem=z_send.at[way, p], recv_sem=z_recv.at[dst_q, p], device_id=(me, there), device_id_type=MESH)

    def line_in(q, p):
        pltpu.make_async_remote_copy(
            src_ref=held[q][p], dst_ref=held[q][p], send_sem=z_send.at[0, p],
            recv_sem=z_recv.at[q, p], device_id=(partner, at), device_id_type=MESH).wait_recv()

    def rows_of(q, u):
        return pl.ds(0, depth) if units[q] == 1 else band(u)

    def slab(side, q, u, column):
        return gathered[side][q].at[:, rows_of(q, u), pl.ds(pl.multiple_of(column * width, 128), width)]

    def across(q, u, j):
        return pltpu.make_async_remote_copy(
            src_ref=picked[q][u].at[j - 1], dst_ref=slab(0, q, u, col), send_sem=c_send.at[q, u, j],
            recv_sem=c_recv.at[q, u, j], device_id=(lax.rem(col + j, cols) * 2 + core, at), device_id_type=MESH)

    def over(q, u, j):
        column = lax.rem(col - j + cols, cols)
        return pltpu.make_async_remote_copy(
            src_ref=slab(0, q, u, column), dst_ref=slab(1, q, u, column), send_sem=p_send.at[q, u, j],
            recv_sem=p_recv.at[q, u, j], device_id=(partner, at), device_id_type=MESH)

    def wanted(column):
        low = (2 * column * bulk + at) * tiles
        high = ((2 * column + 1) * bulk + at) * tiles + tiles - 1
        spots = [low, high] if slots == 2 else [low, low + tiles - 1, high]
        return [irrep_ref[s] for s in spots]

    def spread(q, u):
        src = amp if q == 0 else held[q][u]
        rising = [k + (k >= col).astype(jnp.int32) for k in range(cols - 1)]
        for column in (near[1], near[0], far) if q == 0 else rising:
            j = lax.rem(column - col + cols, cols)
            for s, g in enumerate(wanted(lax.rem(col + j, cols))):
                picked[q][u][j - 1, s] = src[g]
            if q == 0 and column is far:
                pl.semaphore_wait(vouched, 1)
            across(q, u, j).start()
        for s, g in enumerate(mine):
            gathered[0][q][s, rows_of(q, u), pl.ds(pl.multiple_of(col * width, 128), width)] = src[g]
        over(q, u, 0).start()

    def forward(q, only=None):
        for u in range(units[q]) if only is None else only:
            for column in (*near, far):
                j = lax.rem(col - column + cols, cols)
                landed = slab(0, q, u, column)
                pltpu.make_async_remote_copy(
                    src_ref=landed, dst_ref=landed, send_sem=c_send.at[q, u, j], recv_sem=c_recv.at[q, u, j],
                    device_id=(partner, at), device_id_type=MESH).wait_recv()
                over(q, u, j).start()

    first_tile = (me * bulk + at) * tiles

    def product(q, side):
        for t in range(tiles):
            irrep = irrep_ref[first_tile + t]
            slot = (irrep > mine[0]).astype(jnp.int32)
            for s in mine[1:-1]:
                slot = slot + (irrep > s).astype(jnp.int32)
            part = jnp.dot(lhs[plane[q], t], gathered[side][q][slot], preferred_element_type=jnp.float32)
            if q > 0:
                part = part + total[side, t]
            if 0 < q < bulk - 1:
                total[side, t] = part
                continue
            for n in range(cols):
                there = pl.ds(pl.multiple_of((n * 2 + (core if side == 0 else 1 - core)) * width, width), width)
                here = part[:, n * width:(n + 1) * width]
                if q > 0:
                    out_ref[t, :, there] = here.astype(jnp.bfloat16)
                else:
                    total[side, t, :, n * width:(n + 1) * width] = here + res[t, :, there].astype(jnp.float32)

    def arrived(q):
        for u in range(units[q]):
            for j in range(cols):
                over(q, u, j).wait_recv()

    def add(q):
        arrived(q)
        for side in range(2):
            product(q, side)

    for p in range(parts):
        line(0, p).start()

        @pl.when(inner)
        def _():
            line(1, p).start()

    irrep_copy.wait()
    mine = wanted(col)
    spread(0, 0)
    third = jnp.int32(0)
    for column in range(cols):
        for level in range(bulk):
            low = irrep_ref[(2 * column * bulk + level) * tiles]
            high = irrep_ref[((2 * column + 1) * bulk + level) * tiles + tiles - 1]
            third = third + (high > low + 1).astype(jnp.int32)
    flag[0] = third
    flag_copy.start()
    int_copy.wait()
    for k in range(bulk):
        for t in range(tiles):
            lhs[k, t] = ints[t, :, k * depth:(k + 1) * depth]
    res_copy.wait()
    flag_copy.wait()

    for p in range(parts):
        line_in(1, p)

        @pl.when(inner)
        def _():
            line(2, p).start()
            line_in(2, p)
            line(3, p).start()

        spread(1, p)
    for p in range(parts):
        @pl.when(jnp.logical_not(inner))
        def _():
            line_in(2, p)

        spread(2, p)
    @pl.when(inner)
    def _():
        for p in range(parts):
            line_in(3, p)
            line(4, p).start()

    forward(0)
    for p in range(parts):
        @pl.when(jnp.logical_not(inner))
        def _():
            line_in(3, p)

        spread(3, p)
    forward(1)
    add(0)
    forward(2)
    add(1)
    forward(3, range(units[3] - 1))
    add(2)
    forward(3, [units[3] - 1])
    product(3, 0)

    for q in range(bulk):
        for u in range(units[q]):
            for j in range(cols):
                if q < bulk - 1:
                    over(q, u, j).wait_send()
                if j > 0:
                    across(q, u, j).wait_send()
    for p in range(parts):
        line(0, p).wait_send()

        @pl.when(inner)
        def _():
            for way in range(1, 5):
                line(way, p).wait_send()

    arrived(3)
    product(3, 1)
    for u in range(units[3]):
        for j in range(cols):
            over(3, u, j).wait_send()


def call(rows, slots, integrals, amplitudes, residual_in, tile_irrep):
    irreps, depth, width = amplitudes.shape
    tiles, height = integrals.shape[:2]
    parts = 2 if depth % 32 == 0 else 1
    bulk = PLANES
    cols = rows // 2
    hbm = pl.BlockSpec(memory_space=pltpu.HBM)
    kind = amplitudes.dtype
    picked = [depth] + [depth // parts] * (parts * (bulk - 1))
    return pl.pallas_call(
        functools.partial(kernel, rows, slots, parts),
        out_shape=(
            jax.ShapeDtypeStruct(residual_in.shape, residual_in.dtype),
            jax.ShapeDtypeStruct((1,), jnp.int32),
        ),
        in_specs=[hbm] * 4,
        out_specs=(pl.BlockSpec(memory_space=pltpu.VMEM), hbm),
        scratch_shapes=[
            pltpu.SMEM(tile_irrep.shape, tile_irrep.dtype),
            pltpu.SMEM((1,), jnp.int32),
            pltpu.VMEM(amplitudes.shape, kind),
            pltpu.VMEM(integrals.shape, integrals.dtype),
            pltpu.VMEM(residual_in.shape, residual_in.dtype),
            pltpu.VMEM((bulk, tiles, height, depth), integrals.dtype),
            pltpu.VMEM((2, tiles, height, cols * width), jnp.float32),
            *[pltpu.VMEM((slots, depth, cols * width), kind)] * (2 * bulk),
            *[pltpu.VMEM((irreps, depth // parts, width), kind)] * (parts * (bulk - 1)),
            *[pltpu.VMEM((cols - 1, slots, size, width), kind) for size in picked],
            pltpu.SemaphoreType.DMA((5, parts)),
            pltpu.SemaphoreType.DMA((bulk, parts)),
            *[pltpu.SemaphoreType.DMA((bulk, parts, cols))] * 4,
            pltpu.SemaphoreType.DMA((5,)),
            pltpu.SemaphoreType.REGULAR,
        ],
        compiler_params=pltpu.CompilerParams(collective_id=slots, has_side_effects=True, vmem_limit_bytes=VMEM_LIMIT),
    )(tile_irrep, amplitudes, integrals, residual_in)


def local(rows, bulk, integrals, amplitudes, residual_in, tile_irrep):
    depth, width = amplitudes.shape[1:]
    if rows != 2 * COLUMNS or bulk != PLANES or depth % 16 or width % 128:
        return gathered_plan(integrals, amplitudes, residual_in, tile_irrep)
    out, third = call(rows, 2, integrals, amplitudes, residual_in, tile_irrep)
    return lax.cond(
        third[0] > 0,
        lambda out, *args: call(rows, 3, *[pltpu.with_memory_space_constraint(x, pltpu.HBM) for x in args])[0],
        lambda out, *args: out,
        out, integrals, amplitudes, residual_in, tile_irrep)


def solution(mesh):
    return jax.shard_map(
        functools.partial(local, mesh.shape["tile"], mesh.shape["bulk"]),
        mesh=mesh,
        in_specs=(
            P(("tile", "bulk"), None, None),
            P(None, "bulk", "tile"),
            P(("tile", "bulk"), None, None),
            P(),
        ),
        out_specs=P(("tile", "bulk"), None, None),
        check_vma=False,
    )
```
